32 devices in a mesh: ad: 8 (over z, y), tp: 4 (over x, core).
Axes of the slice: x: 2, y: 2, z: 4, core: 2. Of those that a mesh axis runs over, the one named last changes fastest.
Arguments:
- hidden: bfloat16 [256, 8192], P('ad', 'tp'), may hold values from -6 to 6
- queries: bfloat16 [256, 64, 128], P('ad', 'tp'), may hold values from -170 to 170
- key_cache_rows: bfloat16 [256, 8, 128, 128], P('ad', 'tp'), may hold values from -6 to 6
- value_cache_rows: bfloat16 [256, 8, 128, 128], P('ad', 'tp'), may hold values from -6 to 6
- cache_fill_length: int32 [256], P('ad'), may hold values from 1 to 128, as said below
- adapter_choice_index: int32 [256], P('ad'), may hold values from 0 to 511, as said below
- key_value_weight: bfloat16 [8192, 2, 1024], P(None, None, 'tp'), may hold values from -0.0625 to 0.0625
- adapter_down_weight: bfloat16 [512, 16, 8192], P('ad', None, 'tp'), may hold values from -0.0625 to 0.0625
- adapter_up_weight: bfloat16 [512, 16, 2, 1024], P('ad', None, None, 'tp'), may hold values from -1.5 to 1.5
Outputs:
- appended_entries: bfloat16 [256, 2, 8, 128], P('ad', None, 'tp')
- context: bfloat16 [256, 64, 128], P('ad', 'tp')
The draws below stay inside these ranges and needn't reach their ends.
Inputs may be any that keep to these rules, and one draw needn't show every extreme that they name: `adapter_choice_index`: adapter a is held by index a // 64 of ad. Among the 32 sequences of one index of ad, at most 4 name adapters of one holder; in every draw one holder receives exactly 4 from every index of ad. `cache_fill_length`: in every block of 32 sequences one has 128.
All inputs are finite; a program needn't handle non-finite values.
Results may differ from the reference program's by a relative error of at most 0.0053.
Values may be sent and summed in bfloat16 or wider, within the bound.
A program may use at most 128 MiB of HBM per device.

```python
import jax
import jax.numpy as jnp
from jax import lax

MODEL_WIDTH = 8192
HEADS = 64
KEY_VALUE_HEADS = 8
HEAD_WIDTH = 128
ADAPTER_RANK = 16
ADP_DEV = 64
SEQUENCES_LOCAL = 32
CTX = 128
CAP = 4
BATCH_SEQUENCES = 256
ADAPTER_TOTAL = 512


def shared_draw(key):
    lead_keys = jnp.clip(jax.random.normal(jax.random.fold_in(key, 13), (BATCH_SEQUENCES, KEY_VALUE_HEADS, HEAD_WIDTH)), -6.0, 6.0)
    return lead_keys


def draw_key_cache_rows(key, part):
    lead_keys = shared_draw(key)
    all_keys = jnp.clip(jax.random.normal(jax.random.fold_in(key, 14), (BATCH_SEQUENCES, KEY_VALUE_HEADS, CTX, HEAD_WIDTH)), -6.0, 6.0)
    all_keys = all_keys.at[:, :, 0, :].set(lead_keys)
    return all_keys.astype(jnp.bfloat16)


def draw_queries(key, part):
    values_drawn = jnp.clip(jax.random.normal(jax.random.fold_in(key, 15), (BATCH_SEQUENCES, HEADS, HEAD_WIDTH)), -6.0, 6.0)
    return values_drawn.astype(jnp.bfloat16)


def draw_cache_fill_length(key, part):
    block_count_total = BATCH_SEQUENCES // SEQUENCES_LOCAL
    length_rows = jax.random.randint(jax.random.fold_in(key, 21), (block_count_total, SEQUENCES_LOCAL), 1, CTX + 1)
    full_place = jax.random.randint(jax.random.fold_in(key, 22), (block_count_total, 1), 0, SEQUENCES_LOCAL)
    length_rows = jnp.where(jnp.arange(SEQUENCES_LOCAL)[None, :] == full_place, CTX, length_rows)
    return length_rows.reshape(BATCH_SEQUENCES).astype(jnp.int32)


def draw_adapter_choice_index(key, part):
    block_count_total = BATCH_SEQUENCES // SEQUENCES_LOCAL
    cache_slot_count = block_count_total * CAP
    random_noise = jax.random.randint(jax.random.fold_in(key, 31), (block_count_total, cache_slot_count), 0, 65536)
    holder_level = jax.random.randint(jax.random.fold_in(key, 32), (block_count_total,), 0, 4)
    complete_holder = jax.random.randint(jax.random.fold_in(key, 33), (), 0, block_count_total)
    holder_lookup = jnp.arange(cache_slot_count) // CAP
    extra_level = holder_level[holder_lookup] + 8 * (holder_lookup == complete_holder).astype(jnp.int32)
    cache_slot_score = (extra_level[None, :] * 65536 + random_noise) * 1024 + jnp.arange(cache_slot_count)[None, :]
    picked_score, chosen_slots = lax.top_k(cache_slot_score, SEQUENCES_LOCAL)
    owner_rows = chosen_slots // CAP
    shuffle_key = jax.random.randint(jax.random.fold_in(key, 34), (block_count_total, SEQUENCES_LOCAL), 0, 65536) * 1024 + jnp.arange(SEQUENCES_LOCAL)[None, :]
    shuffle_order = jnp.argsort(shuffle_key, axis=1, stable=True)
    owner_rows = jnp.take_along_axis(owner_rows, shuffle_order, axis=1)
    local_index = jax.random.randint(jax.random.fold_in(key, 35), (block_count_total, SEQUENCES_LOCAL), 0, ADP_DEV)
    return (owner_rows * ADP_DEV + local_index).reshape(BATCH_SEQUENCES).astype(jnp.int32)


def block_levels(stream_key, dims, pieces, least, top_value):
    loudness = 1.0
    for position, shards_of in pieces:
        heights = jax.random.uniform(jax.random.fold_in(jax.random.fold_in(stream_key, 6), position), (shards_of,), jnp.float32, least / len(pieces), top_value / len(pieces))
        loudness = loudness * jnp.repeat(jnp.exp(heights), dims[position] // shards_of).reshape((-1,) + (1,) * (len(dims) - 1 - position))
    return loudness


def normal_values(own_key, shape, scale, reach, pieces=(), kind=jnp.bfloat16):
    factor_of = block_levels(own_key, shape, pieces, -0.22, 0.18) if pieces else 1.0
    values = jax.random.normal(own_key, shape, jnp.float32) * scale * factor_of
    return jnp.minimum(jnp.maximum(values, -reach), reach).astype(kind)


def setup_inputs(seed: int = 0) -> dict:
    keys = jax.random.split(jax.random.key(seed), 10)
    hidden = normal_values(keys[0], (BATCH_SEQUENCES, MODEL_WIDTH), 1.0, 6.0, ((0, 8), (1, 4)))
    queries = draw_queries(jax.random.fold_in(keys[9], 71), 0)
    key_cache_rows = draw_key_cache_rows(jax.random.fold_in(keys[9], 71), 0)
    value_cache_rows = normal_values(keys[3], (BATCH_SEQUENCES, KEY_VALUE_HEADS, CTX, HEAD_WIDTH), 1.0, 6.0, ((0, 8), (1, 4)))
    cache_fill_length = draw_cache_fill_length(jax.random.fold_in(keys[9], 71), 0)
    adapter_choice_index = draw_adapter_choice_index(jax.random.fold_in(keys[9], 71), 0)
    key_value_weight = normal_values(keys[6], (MODEL_WIDTH, 2, KEY_VALUE_HEADS * HEAD_WIDTH), MODEL_WIDTH ** -0.5, 0.0625, ((2, 4),))
    adapter_down_weight = normal_values(keys[7], (ADAPTER_TOTAL, ADAPTER_RANK, MODEL_WIDTH), MODEL_WIDTH ** -0.5, 0.0625, ((0, 8), (2, 4)))
    adapter_up_weight = normal_values(keys[8], (ADAPTER_TOTAL, ADAPTER_RANK, 2, KEY_VALUE_HEADS * HEAD_WIDTH), ADAPTER_RANK ** -0.5, 1.5, ((0, 8), (3, 4)))
    return dict(hidden=hidden, queries=queries, key_cache_rows=key_cache_rows, value_cache_rows=value_cache_rows, cache_fill_length=cache_fill_length, adapter_choice_index=adapter_choice_index, key_value_weight=key_value_weight, adapter_down_weight=adapter_down_weight, adapter_up_weight=adapter_up_weight)


adapter_scale = 0.5
epsilon = 1e-05

def attend_block(packed):
    grouped_heads, keys_block, values_block, lengths_block, fresh_block = packed
    inverse_square_root = HEAD_WIDTH ** (-0.5)
    appended_keys = fresh_block[:, 0].astype(jnp.float32)
    new_values = fresh_block[:, 1].astype(jnp.float32)
    scores = jnp.einsum('bkgd,bkcd->bkgc', grouped_heads.astype(jnp.float32), keys_block.astype(jnp.float32)) * inverse_square_root
    self_score = jnp.einsum('rxlw,rxw->rxl', grouped_heads.astype(jnp.float32), appended_keys) * inverse_square_root
    in_cache = jnp.arange(CTX, dtype=jnp.int32)[None, :] < lengths_block[:, None]
    scores = jnp.where(in_cache[:, None, None, :], scores, jnp.float32(-1e+30))
    row_max = jnp.maximum(lax.optimization_barrier(jnp.max(scores, axis=3)), self_score)
    exp_terms = jnp.exp(scores - row_max[..., None])
    own_exp = jnp.exp(self_score - row_max)
    denominator = lax.optimization_barrier(jnp.sum(exp_terms, axis=3)) + own_exp
    weights = (exp_terms / denominator[..., None]).astype(jnp.bfloat16)
    own_weight = (own_exp / denominator).astype(jnp.bfloat16)
    context = jnp.einsum('bkgc,bkcd->bkgd', weights.astype(jnp.float32), values_block.astype(jnp.float32))
    context = context + own_weight.astype(jnp.float32)[..., None] * new_values[:, :, None, :]
    return context.astype(jnp.bfloat16)

def reference(hidden, queries, key_cache_rows, value_cache_rows, cache_fill_length, adapter_choice_index, key_value_weight, adapter_down_weight, adapter_up_weight):
    key_value_columns = 2 * KEY_VALUE_HEADS * HEAD_WIDTH
    widened = hidden.astype(jnp.float32)
    inverse = lax.rsqrt(lax.optimization_barrier(jnp.mean(widened * widened, axis=1, keepdims=True)) + epsilon)
    normed_input = (widened * inverse).astype(jnp.bfloat16)
    plain_projection_rows = jnp.dot(normed_input, key_value_weight.reshape(MODEL_WIDTH, key_value_columns), preferred_element_type=jnp.float32)
    block_count_total = BATCH_SEQUENCES // SEQUENCES_LOCAL

    def adapter_block(packed):
        block_rows, block_index_list = packed
        down_rows = adapter_down_weight[block_index_list].astype(jnp.float32)
        latent_state = jnp.einsum('sd,srd->sr', block_rows.astype(jnp.float32), down_rows).astype(jnp.bfloat16)
        up_rows = adapter_up_weight[block_index_list].reshape(block_index_list.shape[0], ADAPTER_RANK, key_value_columns).astype(jnp.float32)
        return adapter_scale * jnp.einsum('tb,tbl->tl', latent_state.astype(jnp.float32), up_rows)
    adapter_correction = lax.map(adapter_block, (normed_input.reshape(block_count_total, SEQUENCES_LOCAL, MODEL_WIDTH), adapter_choice_index.reshape(block_count_total, SEQUENCES_LOCAL)))
    adapter_correction = adapter_correction.reshape(BATCH_SEQUENCES, key_value_columns)
    appended_entries = (plain_projection_rows + adapter_correction).astype(jnp.bfloat16).reshape(BATCH_SEQUENCES, 2, KEY_VALUE_HEADS, HEAD_WIDTH)
    group_size = HEADS // KEY_VALUE_HEADS
    grouped_heads = queries.reshape(block_count_total, SEQUENCES_LOCAL, KEY_VALUE_HEADS, group_size, HEAD_WIDTH)
    context = lax.map(attend_block, (grouped_heads, key_cache_rows.reshape(block_count_total, SEQUENCES_LOCAL, KEY_VALUE_HEADS, CTX, HEAD_WIDTH), value_cache_rows.reshape(block_count_total, SEQUENCES_LOCAL, KEY_VALUE_HEADS, CTX, HEAD_WIDTH), cache_fill_length.reshape(block_count_total, SEQUENCES_LOCAL), appended_entries.reshape(block_count_total, SEQUENCES_LOCAL, 2, KEY_VALUE_HEADS, HEAD_WIDTH)))
    context = context.reshape(BATCH_SEQUENCES, HEADS, HEAD_WIDTH)
    return (appended_entries, context)
```

```python
import functools

import jax
import jax.numpy as jnp
from jax import lax
from jax.experimental import pallas as pl
from jax.experimental.pallas import tpu as pltpu
from jax.sharding import PartitionSpec as P

MODEL_WIDTH = 8192
CAP = 4
adapter_scale = 0.5
epsilon = 1e-05
LANES = 128
MESH = pl.DeviceIdType.MESH
F32 = jnp.float32
BF16 = jnp.bfloat16


def iota(shape, dim):
    return lax.broadcasted_iota(jnp.int32, shape, dim)


def dot_last(a, b):
    return lax.dot_general(a, b, (((1,), (1,)), ((), ())), preferred_element_type=F32)


def columns(flat):
    n = flat.shape[0] // 32
    runs = flat.reshape(n, 2, 16, LANES)
    first, second = runs[:, 0], runs[:, 1]
    even = lax.rem(iota((n, 16, LANES), 1), 4) < 2
    left = jnp.where(even, first, pltpu.roll(second, 2, 1))
    right = jnp.where(even, pltpu.roll(first, 14, 1), second)
    return jnp.concatenate([left.reshape(n * 16, LANES), right.reshape(n * 16, LANES)], axis=1)


def kernel(
    n_ad, n_tp, rank, width, idx_in, fill_in, hid_in, q_in, k_in, v_in, w_in, dn_in, up_in,
    app_ref, ctx_ref,
    idx_ref, fill_ref, h_all, q_s, k_s, v_s, w_s, dn_s, up_s,
    sb, rb, pb, db, ret, lhs_s, acc_s, m_s, l_s, p_s,
    in_sem, w_sem, own_sem,
    slab_send, slab_recv, row_send, row_recv, lat_send, lat_recv, ret_send, ret_recv,
):
    ad = lax.axis_index("ad")
    tp = lax.axis_index("tp")
    rows, slab = hid_in.shape
    half = slab // 2
    pack_rows = n_ad * 2 * CAP
    adapters = dn_in.shape[0] // rank
    per = LANES // rank
    groups = adapters // per
    head = q_in.shape[2]
    heads = q_in.shape[1]
    kv = k_in.shape[1]
    group = heads // kv
    ctx = k_in.shape[2]
    scale = head ** (-0.5)

    ad_peers = [lax.rem(ad + i, n_ad) for i in range(1, n_ad)]
    tp_peers = [lax.rem(tp + i, n_tp) for i in range(1, n_tp)]
    far = lax.rem(tp + 2, n_tp)
    near = tp + 1 - 2 * lax.rem(tp, 2)

    barrier = pltpu.get_barrier_semaphore()
    for o in ad_peers:
        pl.semaphore_signal(barrier, inc=1, device_id=(o, tp), device_id_type=MESH)
    for t in tp_peers:
        pl.semaphore_signal(barrier, inc=1, device_id=(ad, t), device_id_type=MESH)

    idx_copy = pltpu.make_async_copy(idx_in, idx_ref, in_sem.at[5])
    hid_copy = pltpu.make_async_copy(hid_in, h_all.at[tp], in_sem.at[0])
    fill_copy = pltpu.make_async_copy(fill_in, fill_ref, in_sem.at[6])
    q_copy = pltpu.make_async_copy(q_in, q_s, in_sem.at[1])
    k_copy = pltpu.make_async_copy(k_in, k_s, in_sem.at[2])
    v_copy = pltpu.make_async_copy(v_in, v_s, in_sem.at[3])
    dn_copy = pltpu.make_async_copy(dn_in, dn_s, in_sem.at[4])
    up_copy = pltpu.make_async_copy(up_in, up_s, in_sem.at[7])
    flat_slab = w_in.shape[0] // n_tp
    w_copies = [
        pltpu.make_async_copy(
            w_in.at[pl.ds(i * flat_slab, flat_slab)], w_s.at[pl.ds(i * flat_slab, flat_slab)], w_sem.at[i]
        )
        for i in range(n_tp)
    ]
    for c in (idx_copy, hid_copy, fill_copy, q_copy, k_copy, v_copy, dn_copy, up_copy):
        c.start()

    lane = iota((LANES, 2 * LANES), 0)
    eighth = lax.rem(lane, 8)
    place = 2 * (lane - eighth) + jnp.where(eighth < 4, 4 * eighth, 4 * eighth - 14)
    parity = jnp.concatenate(
        [
            jnp.where(iota((LANES, 2 * LANES), 1) == place + kind, 1.0, 0.0).astype(BF16)
            for kind in range(2)
        ],
        axis=1,
    )

    idx_copy.wait()
    idx_r = jnp.broadcast_to(idx_ref[...].astype(F32), (rows, rows))
    eye = iota((rows, rows), 0) == iota((rows, rows), 1)
    idx_c = jnp.sum(jnp.where(eye, idx_r, 0.0), axis=1, keepdims=True)
    owner_r = jnp.zeros((rows, rows), F32)
    owner_c = jnp.zeros((rows, 1), F32)
    for o in range(1, n_ad):
        owner_r = owner_r + jnp.where(idx_r >= o * adapters, 1.0, 0.0)
        owner_c = owner_c + jnp.where(idx_c >= o * adapters, 1.0, 0.0)
    local_r = idx_r - owner_r * adapters
    same = owner_r == owner_c
    before = iota((rows, rows), 1) < iota((rows, rows), 0)
    after = iota((rows, rows), 0) < iota((rows, rows), 1)
    place_c = jnp.sum(jnp.where(same & before, 1.0, 0.0), axis=1, keepdims=True)
    place_r = jnp.sum(jnp.where(same & after, 1.0, 0.0), axis=0, keepdims=True)
    target_r = owner_r[0:1] * (2 * CAP) + place_r
    target_c = owner_c * (2 * CAP) + place_c
    row_id = iota((pack_rows, rows), 0).astype(F32)
    low = jnp.where(row_id == target_r, 1.0, 0.0)
    high = jnp.where(row_id == target_r + CAP, 1.0, 0.0)
    both = low + high
    ids_out = jnp.sum(both * local_r[0:1], axis=1, keepdims=True) + adapters * (
        1.0 - jnp.sum(both, axis=1, keepdims=True)
    )

    hid_copy.wait()
    mine = h_all[tp]
    packed = jnp.dot(low.astype(BF16), mine[:, :half], preferred_element_type=F32) + jnp.dot(
        high.astype(BF16), mine[:, half:], preferred_element_type=F32
    )
    sb[:, :, 0:half] = packed.reshape(n_ad, 2 * CAP, half).astype(BF16)
    sb[:, :, half : half + LANES] = (
        jnp.broadcast_to(ids_out, (pack_rows, LANES)).reshape(n_ad, 2 * CAP, LANES).astype(BF16)
    )

    pl.semaphore_wait(barrier, n_ad - 1 + n_tp - 1)

    row_copies = []
    for i, o in enumerate(ad_peers):
        row_copies.append(
            pltpu.make_async_remote_copy(
                src_ref=sb.at[o], dst_ref=rb.at[ad], send_sem=row_send.at[i], recv_sem=row_recv.at[i],
                device_id=(o, tp), device_id_type=MESH,
            )
        )
        row_copies[-1].start()
    own_rows = pltpu.make_async_copy(sb.at[ad], rb.at[ad], own_sem.at[0])
    own_rows.start()

    def slab_copy(src, to, n):
        return pltpu.make_async_remote_copy(
            src_ref=h_all.at[src], dst_ref=h_all.at[src], send_sem=slab_send.at[n], recv_sem=slab_recv.at[n],
            device_id=(ad, to), device_id_type=MESH,
        )

    slab_far = slab_copy(tp, far, 0)
    slab_far.start()
    slab_near = slab_copy(tp, near, 1)
    slab_near.start()

    fill_copy.wait()
    q_copy.wait()
    k_copy.wait()
    v_copy.wait()
    for c in w_copies:
        c.start()

    lane_group = iota((heads, kv * ctx), 1)
    head_row = iota((heads, kv * ctx), 0)
    block_ok = jnp.zeros((heads, kv * ctx), jnp.bool_)
    for g in range(kv):
        block_ok = block_ok | (
            (lane_group >= g * ctx) & (lane_group < (g + 1) * ctx)
            & (head_row >= g * group) & (head_row < (g + 1) * group)
        )
    slot = lane_group
    for g in range(1, kv):
        slot = jnp.where(lane_group >= g * ctx, lane_group - g * ctx, slot)
    slot = jnp.where(block_ok, slot, ctx)

    for b in range(rows):
        p_s[b] = jnp.where(
            slot < fill_ref[b], dot_last(q_s[b], k_s[b].reshape(kv * ctx, head)) * scale, -1e30
        )
    for b in range(rows):
        s = p_s[b]
        m = jnp.max(s, axis=1, keepdims=True)
        p = jnp.exp(s - m)
        p_s[b] = p
        m_s[b] = jnp.broadcast_to(m, (heads, head))
        l_s[b] = jnp.broadcast_to(jnp.sum(p, axis=1, keepdims=True), (heads, head))
    for b in range(rows):
        acc_s[b] = jnp.dot(p_s[b].astype(BF16), v_s[b].reshape(kv * ctx, head), preferred_element_type=F32)

    slab_far.wait()
    slab_on = slab_copy(far, near, 2)
    slab_on.start()

    dn_copy.wait()
    own_rows.wait()
    for c in row_copies:
        c.wait()
    wide = rb[:, :, 0:half].astype(F32).reshape(pack_rows, half)
    ids = rb[:, :, half : half + LANES].astype(F32).reshape(pack_rows, LANES)
    got = wide.astype(BF16)
    squares = jnp.sum(wide * wide, axis=1, keepdims=True)
    first = dot_last(got, dn_s[:, 0:half])
    second = dot_last(got, dn_s[:, half:slab])
    sub = iota((n_ad, 2 * CAP, LANES), 1).reshape(pack_rows, LANES)
    is_low = sub < CAP
    lane_adapter = jnp.floor(iota((pack_rows, LANES), 1).astype(F32) * (1.0 / rank))
    latent = jnp.zeros((pack_rows, LANES), F32)
    for t in range(groups):
        part = slice(t * LANES, (t + 1) * LANES)
        pick = jnp.where(is_low, first[:, part], second[:, part])
        latent = latent + jnp.where(ids == lane_adapter + t * per, pick, 0.0)
    mine_lane = lane_adapter == ids - per * jnp.floor(ids * (1.0 / per))
    msg = jnp.where(mine_lane, latent, squares).reshape(n_ad, 2 * CAP, LANES)
    pb[tp] = msg[:, 0:CAP] + msg[:, CAP : 2 * CAP]

    lat_copies = []
    for i, t in enumerate(tp_peers):
        lat_copies.append(
            pltpu.make_async_remote_copy(
                src_ref=pb.at[tp], dst_ref=pb.at[tp], send_sem=lat_send.at[i], recv_sem=lat_recv.at[i],
                device_id=(ad, t), device_id_type=MESH,
            )
        )
        lat_copies[-1].start()

    slab_near.wait()
    slab_on.wait()
    square_sum = jnp.zeros((rows, 1), F32)
    for t in range(n_tp):
        x = h_all[t].astype(F32)
        square_sum = square_sum + jnp.sum(x * x, axis=1, keepdims=True)
    inverse = lax.rsqrt(square_sum / MODEL_WIDTH + epsilon)
    for t in range(n_tp):
        normed = (h_all[t].astype(F32) * inverse).astype(BF16)
        stack = jnp.concatenate([normed[:, j * LANES : (j + 1) * LANES] for j in range(slab // LANES)], axis=0)
        wide_rows = jnp.dot(stack, parity, preferred_element_type=F32).astype(BF16)
        for j in range(slab // LANES):
            at = 2 * (t * slab + j * LANES)
            both = wide_rows[j * rows : (j + 1) * rows]
            lhs_s[0:rows, at : at + 2 * LANES] = both[:, 0 : 2 * LANES]
            lhs_s[rows : 2 * rows, at : at + 2 * LANES] = both[:, 2 * LANES :]
    up_copy.wait()
    up_flat = columns(up_s[...])

    for c in lat_copies:
        c.wait()
    total = pb[0]
    for t in range(1, n_tp):
        total = total + pb[t]
    total = jnp.concatenate([total, total], axis=1).reshape(pack_rows, LANES)
    square_sum = jnp.max(jnp.where(mine_lane, 0.0, total), axis=1, keepdims=True)
    latent = total * lax.rsqrt(square_sum / MODEL_WIDTH + epsilon)
    latent = jnp.dot(
        jnp.where(mine_lane, latent, 0.0).astype(BF16), parity, preferred_element_type=F32
    )
    wide_low = iota((n_ad, 2 * CAP, 2 * LANES), 1).reshape(pack_rows, 2 * LANES) < CAP
    latent = jnp.where(wide_low, latent[:, 0 : 2 * LANES], latent[:, 2 * LANES :])
    wide_ids = jnp.concatenate([ids, ids], axis=1)
    wide_adapter = jnp.floor(iota((pack_rows, 2 * LANES), 1).astype(F32) * (0.5 / rank))
    spread = jnp.concatenate(
        [jnp.where(wide_ids == wide_adapter + t * per, latent, 0.0).astype(BF16) for t in range(groups)], axis=1
    )
    delta = adapter_scale * jnp.dot(spread, up_flat, preferred_element_type=F32)
    db[...] = delta.reshape(n_ad, 2 * CAP, width)

    ret_copies = []
    for i, o in enumerate(ad_peers):
        ret_copies.append(
            pltpu.make_async_remote_copy(
                src_ref=db.at[o], dst_ref=ret.at[ad], send_sem=ret_send.at[i], recv_sem=ret_recv.at[i],
                device_id=(o, tp), device_id_type=MESH,
            )
        )
        ret_copies[-1].start()
    own_ret = pltpu.make_async_copy(db.at[ad], ret.at[ad], own_sem.at[1])
    own_ret.start()

    base = jnp.zeros((2 * rows, width), F32)
    piece = slab // 4
    for t in range(n_tp):
        w_copies[t].wait()
        for j in range(4):
            at = t * slab + j * piece
            flat = columns(w_s[4 * at : 4 * (at + piece)])
            base = base + jnp.dot(lhs_s[:, 2 * at : 2 * (at + piece)], flat, preferred_element_type=F32)

    pick_id = iota((rows, pack_rows), 1).astype(F32)
    own_ret.wait()
    for c in ret_copies:
        c.wait()
    back = ret[...].reshape(pack_rows, width)
    pick = jnp.concatenate(
        [jnp.where(pick_id == target_c + kind * CAP, 1.0, 0.0) for kind in range(2)], axis=0
    )
    moved = jnp.dot(pick, back, precision=lax.Precision.HIGHEST, preferred_element_type=F32)
    new = (base + moved).astype(BF16)
    app_ref[0] = new[0:rows]
    app_ref[1] = new[rows : 2 * rows]
    new = new.astype(F32)
    fresh = (new[0:rows], new[rows : 2 * rows])
    for b in range(rows):
        key_rows, value_rows = (
            jnp.concatenate(
                [jnp.broadcast_to(f[b : b + 1, g * head : (g + 1) * head], (group, head)) for g in range(kv)], axis=0
            )
            for f in fresh
        )
        own = jnp.sum(q_s[b].astype(F32) * key_rows, axis=1, keepdims=True) * scale
        m = m_s[b]
        top = jnp.maximum(m, own)
        keep = jnp.exp(m - top)
        own_exp = jnp.exp(own - top)
        ctx_ref[b] = ((acc_s[b] * keep + own_exp * value_rows) / (l_s[b] * keep + own_exp)).astype(BF16)


def by_tile(a):
    tiles = a.shape[-1] // LANES
    return a.reshape(-1, 2, tiles, LANES).transpose(0, 2, 1, 3).reshape(-1, LANES)


def on_device(n_ad, n_tp, hidden, queries, keys, values, fill, choice, weight, down, up):
    rows, slab = hidden.shape
    adapters, rank, _ = down.shape
    width = up.shape[3]
    heads, head = queries.shape[1:]
    kv = keys.shape[1]
    pack_rows = 2 * CAP
    any_spec = pl.BlockSpec(memory_space=pl.ANY)
    vmem = pl.BlockSpec(memory_space=pltpu.VMEM)
    app, ctx = pl.pallas_call(
        functools.partial(kernel, n_ad, n_tp, rank, width),
        out_shape=(
            jax.ShapeDtypeStruct((2, rows, width), BF16),
            jax.ShapeDtypeStruct(queries.shape, BF16),
        ),
        in_specs=[any_spec] * 9,
        out_specs=(vmem, vmem),
        scratch_shapes=[
            pltpu.VMEM((1, rows), jnp.int32),
            pltpu.SMEM((rows,), jnp.int32),
            pltpu.VMEM((n_tp, rows, slab), BF16),
            pltpu.VMEM(queries.shape, BF16),
            pltpu.VMEM(keys.shape, BF16),
            pltpu.VMEM(values.shape, BF16),
            pltpu.VMEM((4 * weight.shape[0], LANES), BF16),
            pltpu.VMEM((adapters * rank, slab), BF16),
            pltpu.VMEM((4 * adapters * rank, LANES), BF16),
            pltpu.VMEM((n_ad, pack_rows, slab // 2 + LANES), BF16),
            pltpu.VMEM((n_ad, pack_rows, slab // 2 + LANES), BF16),
            pltpu.VMEM((n_tp, n_ad, CAP, LANES), F32),
            pltpu.VMEM((n_ad, pack_rows, width), F32),
            pltpu.VMEM((n_ad, pack_rows, width), F32),
            pltpu.VMEM((2 * rows, 2 * weight.shape[0]), BF16),
            pltpu.VMEM(queries.shape, F32),
            pltpu.VMEM(queries.shape, F32),
            pltpu.VMEM(queries.shape, F32),
            pltpu.VMEM((rows, heads, kv * keys.shape[2]), F32),
            pltpu.SemaphoreType.DMA((8,)),
            pltpu.SemaphoreType.DMA((n_tp,)),
            pltpu.SemaphoreType.DMA((2,)),
            pltpu.SemaphoreType.DMA((3,)),
            pltpu.SemaphoreType.DMA((3,)),
            pltpu.SemaphoreType.DMA((n_ad - 1,)),
            pltpu.SemaphoreType.DMA((n_ad - 1,)),
            pltpu.SemaphoreType.DMA((n_tp - 1,)),
            pltpu.SemaphoreType.DMA((n_tp - 1,)),
            pltpu.SemaphoreType.DMA((n_ad - 1,)),
            pltpu.SemaphoreType.DMA((n_ad - 1,)),
        ],
        compiler_params=pltpu.CompilerParams(
            collective_id=0, has_side_effects=True, vmem_limit_bytes=40 * 1024 * 1024
        ),
    )(*[
        pltpu.with_memory_space_constraint(x, pltpu.HBM)
        for x in (
            choice.reshape(1, rows), fill, hidden, queries, keys, values,
            by_tile(weight),
            down.reshape(adapters * rank, slab),
            by_tile(up),
        )
    ])

    def finish(app_ref, ctx_ref, app_out, ctx_out):
        for kind in range(2):
            for g in range(kv):
                app_out[:, kind, g, :] = app_ref[kind, :, g * head : (g + 1) * head]
        ctx_out[...] = ctx_ref[...]

    return pl.pallas_call(
        finish,
        out_shape=(
            jax.ShapeDtypeStruct((rows, 2, kv, head), BF16),
            jax.ShapeDtypeStruct(queries.shape, BF16),
        ),
        in_specs=[vmem] * 2,
        out_specs=(vmem, vmem),
        compiler_params=pltpu.CompilerParams(vmem_limit_bytes=4 * 1024 * 1024),
    )(app, ctx)


def solution(mesh):
    placed = (
        P("ad", "tp"),
        P("ad", "tp", None),
        P("ad", "tp", None, None),
        P("ad", "tp", None, None),
        P("ad"),
        P("ad"),
        P(None, None, "tp"),
        P("ad", None, "tp"),
        P("ad", None, None, "tp"),
    )
    return jax.shard_map(
        functools.partial(on_device, mesh.shape["ad"], mesh.shape["tp"]),
        mesh=mesh,
        in_specs=placed,
        out_specs=(P("ad", None, "tp", None), P("ad", "tp", None)),
        check_vma=False,
    )
```

```python
import functools

import jax
import jax.numpy as jnp
from jax import lax
from jax.experimental import pallas as pl
from jax.experimental.pallas import tpu as pltpu
from jax.sharding import PartitionSpec as P

MODEL_WIDTH = 8192
CAP = 4
adapter_scale = 0.5
epsilon = 1e-05
LANES = 128
MESH = pl.DeviceIdType.MESH
F32 = jnp.float32
BF16 = jnp.bfloat16


def iota(shape, dim):
    return lax.broadcasted_iota(jnp.int32, shape, dim)


def dot_last(a, b):
    return lax.dot_general(a, b, (((1,), (1,)), ((), ())), preferred_element_type=F32)


def columns(flat):
    n = flat.shape[0] // 32
    runs = flat.reshape(n, 2, 16, LANES)
    first, second = runs[:, 0], runs[:, 1]
    even = lax.rem(iota((n, 16, LANES), 1), 4) < 2
    left = jnp.where(even, first, pltpu.roll(second, 2, 1))
    right = jnp.where(even, pltpu.roll(first, 14, 1), second)
    return jnp.concatenate([left.reshape(n * 16, LANES), right.reshape(n * 16, LANES)], axis=1)


def landed(ref, sem):
    pltpu.make_async_copy(ref, ref, sem).wait()


def kernel(
    n_ad, n_tp, rank, width, idx_in, fill_in, hid_in, q_in, k_in, v_in, w_in, dn_in, up_in,
    app_ref, ctx_ref,
    idx_ref, fill_ref, h_all, q_s, k_s, v_s, w_s, dn_s, dn_t, up_s,
    sb, rb, pb, db, ret, lhs_s, acc_s, m_s, l_s, p_s,
    in_sem, w_sem, slab_sem, row_sem, lat_sem, ret_sem,
):
    ad = lax.axis_index("ad")
    tp = lax.axis_index("tp")
    rows, slab = hid_in.shape
    half = slab // 2
    pack_rows = n_ad * 2 * CAP
    adapters = dn_in.shape[0] // rank
    per = LANES // rank
    groups = adapters // per
    head = q_in.shape[2]
    heads = q_in.shape[1]
    kv = k_in.shape[1]
    group = heads // kv
    ctx = k_in.shape[2]
    scale = head ** (-0.5)

    ad_peers = [lax.rem(ad + i, n_ad) for i in range(n_ad - 1, 0, -1)]
    tp_peers = [lax.rem(tp + i, n_tp) for i in range(1, n_tp)]
    far = lax.rem(tp + 2, n_tp)
    near = tp + 1 - 2 * lax.rem(tp, 2)

    barrier = pltpu.get_barrier_semaphore()
    for o in ad_peers:
        pl.semaphore_signal(barrier, inc=1, device_id=(o, tp), device_id_type=MESH)
    for t in tp_peers:
        pl.semaphore_signal(barrier, inc=1, device_id=(ad, t), device_id_type=MESH)

    idx_copy = pltpu.make_async_copy(idx_in, idx_ref, in_sem.at[5])
    hid_copy = pltpu.make_async_copy(hid_in, h_all.at[tp], in_sem.at[0])
    fill_copy = pltpu.make_async_copy(fill_in, fill_ref, in_sem.at[6])
    q_copy = pltpu.make_async_copy(q_in, q_s, in_sem.at[1])
    k_copy = pltpu.make_async_copy(k_in, k_s, in_sem.at[2])
    v_copy = pltpu.make_async_copy(v_in, v_s, in_sem.at[3])
    dn_copy = pltpu.make_async_copy(dn_in, dn_s, in_sem.at[4])
    up_copy = pltpu.make_async_copy(up_in, up_s, in_sem.at[7])
    flat_slab = w_in.shape[0] // n_tp
    w_copies = [
        pltpu.make_async_copy(
            w_in.at[pl.ds(i * flat_slab, flat_slab)], w_s.at[pl.ds(i * flat_slab, flat_slab)], w_sem.at[i]
        )
        for i in range(n_tp)
    ]
    for c in (idx_copy, hid_copy, fill_copy, q_copy, k_copy, v_copy, dn_copy, up_copy):
        c.start()

    lane = iota((LANES, 2 * LANES), 0)
    eighth = lax.rem(lane, 8)
    place = 2 * (lane - eighth) + jnp.where(eighth < 4, 4 * eighth, 4 * eighth - 14)
    parity = jnp.concatenate(
        [
            jnp.where(iota((LANES, 2 * LANES), 1) == place + kind, 1.0, 0.0).astype(BF16)
            for kind in range(2)
        ],
        axis=1,
    )

    idx_copy.wait()
    idx_r = jnp.broadcast_to(idx_ref[...].astype(F32), (rows, rows))
    eye = iota((rows, rows), 0) == iota((rows, rows), 1)
    idx_c = jnp.sum(jnp.where(eye, idx_r, 0.0), axis=1, keepdims=True)
    owner_r = jnp.zeros((rows, rows), F32)
    owner_c = jnp.zeros((rows, 1), F32)
    for o in range(1, n_ad):
        owner_r = owner_r + jnp.where(idx_r >= o * adapters, 1.0, 0.0)
        owner_c = owner_c + jnp.where(idx_c >= o * adapters, 1.0, 0.0)
    local_r = idx_r - owner_r * adapters
    same = owner_r == owner_c
    before = iota((rows, rows), 1) < iota((rows, rows), 0)
    after = iota((rows, rows), 0) < iota((rows, rows), 1)
    place_c = jnp.sum(jnp.where(same & before, 1.0, 0.0), axis=1, keepdims=True)
    place_r = jnp.sum(jnp.where(same & after, 1.0, 0.0), axis=0, keepdims=True)
    target_r = owner_r[0:1] * (2 * CAP) + place_r
    target_c = owner_c * (2 * CAP) + place_c
    row_id = iota((pack_rows, rows), 0).astype(F32)
    low = jnp.where(row_id == target_r, 1.0, 0.0)
    high = jnp.where(row_id == target_r + CAP, 1.0, 0.0)
    both = low + high
    ids_out = jnp.sum(both * local_r[0:1], axis=1, keepdims=True) + adapters * (
        1.0 - jnp.sum(both, axis=1, keepdims=True)
    )

    hid_copy.wait()
    mine = h_all[tp]
    packed = jnp.dot(low.astype(BF16), mine[:, :half], preferred_element_type=F32) + jnp.dot(
        high.astype(BF16), mine[:, half:], preferred_element_type=F32
    )
    packed = packed.reshape(n_ad, 2 * CAP, half).astype(BF16)
    sb[:, :, 0:half] = packed
    sb[:, :, half : half + LANES] = (
        jnp.broadcast_to(ids_out, (pack_rows, LANES)).reshape(n_ad, 2 * CAP, LANES).astype(BF16)
    )

    pl.semaphore_wait(barrier, n_ad - 1 + n_tp - 1)

    row_copies = []
    for i, o in enumerate(ad_peers):
        row_copies.append(
            pltpu.make_async_remote_copy(
                src_ref=sb.at[o], dst_ref=rb.at[ad], send_sem=row_sem.at[0], recv_sem=row_sem.at[1],
                device_id=(o, tp), device_id_type=MESH,
            )
        )
        row_copies[-1].start()
    own_rows = pltpu.make_async_copy(sb.at[ad], rb.at[ad], row_sem.at[1])
    own_rows.start()

    def slab_copy(src, to, n):
        return pltpu.make_async_remote_copy(
            src_ref=h_all.at[src], dst_ref=h_all.at[src], send_sem=slab_sem.at[3], recv_sem=slab_sem.at[n],
            device_id=(ad, to), device_id_type=MESH,
        )

    slab_far = slab_copy(tp, far, 0)
    slab_far.start()
    slab_near = slab_copy(tp, near, 1)
    slab_near.start()

    fill_copy.wait()
    q_copy.wait()
    k_copy.wait()
    v_copy.wait()
    for c in w_copies:
        c.start()

    lane_group = iota((heads, kv * ctx), 1)
    head_row = iota((heads, kv * ctx), 0)
    block_ok = jnp.zeros((heads, kv * ctx), jnp.bool_)
    for g in range(kv):
        block_ok = block_ok | (
            (lane_group >= g * ctx) & (lane_group < (g + 1) * ctx)
            & (head_row >= g * group) & (head_row < (g + 1) * group)
        )
    slot = lane_group
    for g in range(1, kv):
        slot = jnp.where(lane_group >= g * ctx, lane_group - g * ctx, slot)
    slot = jnp.where(block_ok, slot, ctx)

    for b in range(rows):
        p_s[b] = jnp.where(
            slot < fill_ref[b], dot_last(q_s[b], k_s[b].reshape(kv * ctx, head)) * scale, -1e30
        )
    for b in range(rows):
        s = p_s[b]
        m = jnp.max(s, axis=1, keepdims=True)
        p = jnp.exp(s - m)
        p_s[b] = p
        m_s[b] = jnp.broadcast_to(m, (heads, head))
        l_s[b] = jnp.broadcast_to(jnp.sum(p, axis=1, keepdims=True), (heads, head))
    for b in range(rows):
        acc_s[b] = jnp.dot(p_s[b].astype(BF16), v_s[b].reshape(kv * ctx, head), preferred_element_type=F32)

    dn_copy.wait()
    for j in range(slab // LANES):
        dn_t[j * LANES : (j + 1) * LANES] = dn_s[:, j * LANES : (j + 1) * LANES].T

    slab_far.wait_recv()
    slab_on = slab_copy(far, near, 2)
    slab_on.start()

    sub = iota((n_ad, 2 * CAP, LANES), 1).reshape(pack_rows, LANES)
    is_low = sub < CAP
    lane_adapter = jnp.floor(iota((pack_rows, LANES), 1).astype(F32) * (1.0 / rank))
    landed(rb, row_sem.at[1])
    wide = rb[:, :, 0:half].astype(F32).reshape(pack_rows, half)
    ids = rb[:, :, half : half + LANES].astype(F32).reshape(pack_rows, LANES)
    got = wide.astype(BF16)
    first = jnp.dot(got, dn_t[0:half], preferred_element_type=F32)
    second = jnp.dot(got, dn_t[half:slab], preferred_element_type=F32)
    squares = jnp.sum(wide * wide, axis=1, keepdims=True)
    latent = jnp.zeros((pack_rows, LANES), F32)
    for t in range(groups):
        part = slice(t * LANES, (t + 1) * LANES)
        pick = jnp.where(is_low, first[:, part], second[:, part])
        latent = latent + jnp.where(ids == lane_adapter + t * per, pick, 0.0)
    mine_lane = lane_adapter == ids - per * jnp.floor(ids * (1.0 / per))
    msg = jnp.where(mine_lane, latent, squares).reshape(n_ad, 2 * CAP, LANES)
    pb[tp] = msg[:, 0:CAP] + msg[:, CAP : 2 * CAP]

    lat_copies = []
    for i, t in enumerate(tp_peers):
        lat_copies.append(
            pltpu.make_async_remote_copy(
                src_ref=pb.at[tp], dst_ref=pb.at[tp], send_sem=lat_sem.at[0], recv_sem=lat_sem.at[1],
                device_id=(ad, t), device_id_type=MESH,
            )
        )
        lat_copies[-1].start()

    slab_near.wait_recv()
    slab_on.wait_recv()
    square_sum = jnp.zeros((rows, 1), F32)
    for t in range(n_tp):
        x = h_all[t].astype(F32)
        square_sum = square_sum + jnp.sum(x * x, axis=1, keepdims=True)
    inverse = lax.rsqrt(square_sum / MODEL_WIDTH + epsilon)
    for t in range(n_tp):
        normed = (h_all[t].astype(F32) * inverse).astype(BF16)
        stack = jnp.concatenate([normed[:, j * LANES : (j + 1) * LANES] for j in range(slab // LANES)], axis=0)
        wide_rows = jnp.dot(stack, parity, preferred_element_type=F32).astype(BF16)
        for j in range(slab // LANES):
            at = 2 * (t * slab + j * LANES)
            both = wide_rows[j * rows : (j + 1) * rows]
            lhs_s[0:rows, at : at + 2 * LANES] = both[:, 0 : 2 * LANES]
            lhs_s[rows : 2 * rows, at : at + 2 * LANES] = both[:, 2 * LANES :]
    up_copy.wait()
    up_both = [[], []]
    for t in range(groups):
        flat = columns(up_s[4 * t * LANES : 4 * (t + 1) * LANES])
        for kind in range(2):
            up_both[kind].append(
                lax.dot_general(
                    parity[:, 2 * kind * LANES : 2 * (kind + 1) * LANES], flat, (((1,), (0,)), ((), ())),
                    preferred_element_type=F32,
                ).astype(BF16)
            )
    up_both = [jnp.concatenate(u, axis=0) for u in up_both]

    landed(pb.at[pl.ds(0, n_tp - 1)], lat_sem.at[1])
    total = pb[0]
    for t in range(1, n_tp):
        total = total + pb[t]
    total = jnp.concatenate([total, total], axis=1).reshape(pack_rows, LANES)
    square_sum = jnp.max(jnp.where(mine_lane, 0.0, total), axis=1, keepdims=True)
    latent = total * lax.rsqrt(square_sum / MODEL_WIDTH + epsilon)
    latent = jnp.where(mine_lane, latent, 0.0).astype(BF16)
    spread = jnp.concatenate(
        [jnp.where(ids == lane_adapter + t * per, latent, jnp.zeros_like(latent)) for t in range(groups)], axis=1
    )
    key_delta, value_delta = (jnp.dot(spread, u, preferred_element_type=F32) for u in up_both)
    is_key = iota((n_ad, 2 * CAP, width), 1).reshape(pack_rows, width) < CAP
    delta = adapter_scale * jnp.where(is_key, key_delta, value_delta)
    db[...] = delta.reshape(n_ad, 2 * CAP, width).astype(BF16)

    ret_copies = []
    for i, o in enumerate(ad_peers):
        ret_copies.append(
            pltpu.make_async_remote_copy(
                src_ref=db.at[o], dst_ref=ret.at[ad], send_sem=ret_sem.at[0], recv_sem=ret_sem.at[1],
                device_id=(o, tp), device_id_type=MESH,
            )
        )
        ret_copies[-1].start()
    own_ret = pltpu.make_async_copy(db.at[ad], ret.at[ad], ret_sem.at[1])
    own_ret.start()

    base = jnp.zeros((2 * rows, width), F32)
    piece = slab // 4
    for t in range(n_tp):
        w_copies[t].wait()
        for j in range(4):
            at = t * slab + j * piece
            flat = columns(w_s[4 * at : 4 * (at + piece)])
            base = base + jnp.dot(lhs_s[:, 2 * at : 2 * (at + piece)], flat, preferred_element_type=F32)

    pick_id = iota((rows, pack_rows), 1).astype(F32)
    landed(sb.at[pl.ds(0, n_ad - 1)], row_sem.at[0])
    landed(pb.at[pl.ds(0, n_tp - 1)], lat_sem.at[0])
    landed(h_all.at[pl.ds(0, n_tp - 1)], slab_sem.at[3])
    landed(db.at[pl.ds(0, n_ad - 1)], ret_sem.at[0])
    landed(ret, ret_sem.at[1])
    back = ret[...].astype(F32).reshape(pack_rows, width).astype(BF16)
    pick = jnp.concatenate(
        [jnp.where(pick_id == target_c + kind * CAP, 1.0, 0.0) for kind in range(2)], axis=0
    ).astype(BF16)
    moved = jnp.dot(pick, back, preferred_element_type=F32)
    new = (base + moved).astype(BF16)
    app_ref[0] = new[0:rows]
    app_ref[1] = new[rows : 2 * rows]
    new = new.astype(F32)
    fresh = (new[0:rows], new[rows : 2 * rows])
    for b in range(rows):
        key_rows, value_rows = (
            jnp.concatenate(
                [jnp.broadcast_to(f[b : b + 1, g * head : (g + 1) * head], (group, head)) for g in range(kv)], axis=0
            )
            for f in fresh
        )
        own = jnp.sum(q_s[b].astype(F32) * key_rows, axis=1, keepdims=True) * scale
        m = m_s[b]
        top = jnp.maximum(m, own)
        keep = jnp.exp(m - top)
        own_exp = jnp.exp(own - top)
        ctx_ref[b] = ((acc_s[b] * keep + own_exp * value_rows) / (l_s[b] * keep + own_exp)).astype(BF16)


def by_tile(a):
    tiles = a.shape[-1] // LANES
    return a.reshape(-1, 2, tiles, LANES).transpose(0, 2, 1, 3).reshape(-1, LANES)


def on_device(n_ad, n_tp, hidden, queries, keys, values, fill, choice, weight, down, up):
    rows, slab = hidden.shape
    adapters, rank, _ = down.shape
    width = up.shape[3]
    heads, head = queries.shape[1:]
    kv = keys.shape[1]
    pack_rows = 2 * CAP
    any_spec = pl.BlockSpec(memory_space=pl.ANY)
    vmem = pl.BlockSpec(memory_space=pltpu.VMEM)
    app, ctx = pl.pallas_call(
        functools.partial(kernel, n_ad, n_tp, rank, width),
        out_shape=(
            jax.ShapeDtypeStruct((2, rows, width), BF16),
            jax.ShapeDtypeStruct(queries.shape, BF16),
        ),
        in_specs=[any_spec] * 9,
        out_specs=(vmem, vmem),
        scratch_shapes=[
            pltpu.VMEM((1, rows), jnp.int32),
            pltpu.SMEM((rows,), jnp.int32),
            pltpu.VMEM((n_tp, rows, slab), BF16),
            pltpu.VMEM(queries.shape, BF16),
            pltpu.VMEM(keys.shape, BF16),
            pltpu.VMEM(values.shape, BF16),
            pltpu.VMEM((4 * weight.shape[0], LANES), BF16),
            pltpu.VMEM((adapters * rank, slab), BF16),
            pltpu.VMEM((slab, adapters * rank), BF16),
            pltpu.VMEM((4 * adapters * rank, LANES), BF16),
            pltpu.VMEM((n_ad, pack_rows, slab // 2 + LANES), BF16),
            pltpu.VMEM((n_ad, pack_rows, slab // 2 + LANES), BF16),
            pltpu.VMEM((n_tp, n_ad, CAP, LANES), F32),
            pltpu.VMEM((n_ad, pack_rows, width), BF16),
            pltpu.VMEM((n_ad, pack_rows, width), BF16),
            pltpu.VMEM((2 * rows, 2 * weight.shape[0]), BF16),
            pltpu.VMEM(queries.shape, F32),
            pltpu.VMEM(queries.shape, F32),
            pltpu.VMEM(queries.shape, F32),
            pltpu.VMEM((rows, heads, kv * keys.shape[2]), F32),
            pltpu.SemaphoreType.DMA((8,)),
            pltpu.SemaphoreType.DMA((n_tp,)),
            pltpu.SemaphoreType.DMA((4,)),
            pltpu.SemaphoreType.DMA((2,)),
            pltpu.SemaphoreType.DMA((2,)),
            pltpu.SemaphoreType.DMA((2,)),
        ],
        compiler_params=pltpu.CompilerParams(
            collective_id=0, has_side_effects=True, vmem_limit_bytes=40 * 1024 * 1024
        ),
    )(*[
        pltpu.with_memory_space_constraint(x, pltpu.HBM)
        for x in (
            choice.reshape(1, rows), fill, hidden, queries, keys, values,
            by_tile(weight),
            down.reshape(adapters * rank, slab),
            by_tile(up),
        )
    ])

    def finish(app_ref, ctx_ref, app_out, ctx_out):
        for kind in range(2):
            for g in range(kv):
                app_out[:, kind, g, :] = app_ref[kind, :, g * head : (g + 1) * head]
        ctx_out[...] = ctx_ref[...]

    return pl.pallas_call(
        finish,
        out_shape=(
            jax.ShapeDtypeStruct((rows, 2, kv, head), BF16),
            jax.ShapeDtypeStruct(queries.shape, BF16),
        ),
        in_specs=[vmem] * 2,
        out_specs=(vmem, vmem),
        compiler_params=pltpu.CompilerParams(vmem_limit_bytes=4 * 1024 * 1024),
    )(app, ctx)


def solution(mesh):
    placed = (
        P("ad", "tp"),
        P("ad", "tp", None),
        P("ad", "tp", None, None),
        P("ad", "tp", None, None),
        P("ad"),
        P("ad"),
        P(None, None, "tp"),
        P("ad", None, "tp"),
        P("ad", None, None, "tp"),
    )
    return jax.shard_map(
        functools.partial(on_device, mesh.shape["ad"], mesh.shape["tp"]),
        mesh=mesh,
        in_specs=placed,
        out_specs=(P("ad", None, "tp", None), P("ad", "tp", None)),
        check_vma=False,
    )
```

```python
import functools

import jax
import jax.numpy as jnp
from jax import lax
from jax.experimental import pallas as pl
from jax.experimental.pallas import tpu as pltpu
from jax.sharding import PartitionSpec as P

MODEL_WIDTH = 8192
CAP = 4
adapter_scale = 0.5
epsilon = 1e-05
LANES = 128
MESH = pl.DeviceIdType.MESH
F32 = jnp.float32
BF16 = jnp.bfloat16


def iota(shape, dim):
    return lax.broadcasted_iota(jnp.int32, shape, dim)


def dot_last(a, b):
    return lax.dot_general(a, b, (((1,), (1,)), ((), ())), preferred_element_type=F32)


def columns(flat):
    n = flat.shape[0] // 32
    runs = flat.reshape(n, 2, 16, LANES)
    first, second = runs[:, 0], runs[:, 1]
    even = lax.rem(iota((n, 16, LANES), 1), 4) < 2
    left = jnp.where(even, first, pltpu.roll(second, 2, 1))
    right = jnp.where(even, pltpu.roll(first, 14, 1), second)
    return jnp.concatenate([left.reshape(n * 16, LANES), right.reshape(n * 16, LANES)], axis=1)


def landed(ref, sem):
    pltpu.make_async_copy(ref, ref, sem).wait()


def kernel(
    n_ad, n_tp, rank, width, idx_in, fill_in, hid_in, q_in, k_in, v_in, w_in, dn_in, up_in,
    app_ref, ctx_ref,
    idx_ref, fill_ref, h_all, q_s, k_s, v_s, w_s, dn_s, dn_t, up_s,
    sb, rb, pb, db, ret, lhs_s, acc_s, m_s, l_s, p_s,
    in_sem, w_sem, slab_sem, row_sem, lat_sem, ret_sem,
):
    ad = lax.axis_index("ad")
    tp = lax.axis_index("tp")
    rows, slab = hid_in.shape
    half = slab // 2
    pack_rows = n_ad * 2 * CAP
    adapters = dn_in.shape[0] // rank
    per = LANES // rank
    groups = adapters // per
    head = q_in.shape[2]
    heads = q_in.shape[1]
    kv = k_in.shape[1]
    group = heads // kv
    ctx = k_in.shape[2]
    scale = head ** (-0.5)

    ad_peers = [lax.rem(ad + i, n_ad) for i in range(n_ad - 1, 0, -1)]
    tp_peers = [lax.rem(tp + i, n_tp) for i in range(1, n_tp)]
    far = lax.rem(tp + 2, n_tp)
    near = tp + 1 - 2 * lax.rem(tp, 2)

    barrier = pltpu.get_barrier_semaphore()
    for o in ad_peers:
        pl.semaphore_signal(barrier, inc=1, device_id=(o, tp), device_id_type=MESH)
    for t in tp_peers:
        pl.semaphore_signal(barrier, inc=1, device_id=(ad, t), device_id_type=MESH)

    idx_copy = pltpu.make_async_copy(idx_in, idx_ref, in_sem.at[5])
    hid_copy = pltpu.make_async_copy(hid_in, h_all.at[tp], in_sem.at[0])
    fill_copy = pltpu.make_async_copy(fill_in, fill_ref, in_sem.at[6])
    q_copy = pltpu.make_async_copy(q_in, q_s, in_sem.at[1])
    k_copy = pltpu.make_async_copy(k_in, k_s, in_sem.at[2])
    v_copy = pltpu.make_async_copy(v_in, v_s, in_sem.at[3])
    dn_copy = pltpu.make_async_copy(dn_in, dn_s, in_sem.at[4])
    up_copy = pltpu.make_async_copy(up_in, up_s, in_sem.at[7])
    flat_slab = w_in.shape[0] // n_tp
    w_copies = [
        pltpu.make_async_copy(
            w_in.at[pl.ds(i * flat_slab, flat_slab)], w_s.at[pl.ds(i * flat_slab, flat_slab)], w_sem.at[i]
        )
        for i in range(n_tp)
    ]
    for c in (idx_copy, hid_copy, fill_copy, q_copy, k_copy, v_copy, dn_copy, up_copy):
        c.start()

    lane = iota((LANES, 2 * LANES), 0)
    eighth = lax.rem(lane, 8)
    place = 2 * (lane - eighth) + jnp.where(eighth < 4, 4 * eighth, 4 * eighth - 14)
    parity = jnp.concatenate(
        [
            jnp.where(iota((LANES, 2 * LANES), 1) == place + kind, 1.0, 0.0).astype(BF16)
            for kind in range(2)
        ],
        axis=1,
    )

    idx_copy.wait()
    idx_r = jnp.broadcast_to(idx_ref[...].astype(F32), (rows, rows))
    eye = iota((rows, rows), 0) == iota((rows, rows), 1)
    idx_c = jnp.sum(jnp.where(eye, idx_r, 0.0), axis=1, keepdims=True)
    owner_r = jnp.zeros((rows, rows), F32)
    owner_c = jnp.zeros((rows, 1), F32)
    for o in range(1, n_ad):
        owner_r = owner_r + jnp.where(idx_r >= o * adapters, 1.0, 0.0)
        owner_c = owner_c + jnp.where(idx_c >= o * adapters, 1.0, 0.0)
    local_r = idx_r - owner_r * adapters
    same = owner_r == owner_c
    before = iota((rows, rows), 1) < iota((rows, rows), 0)
    after = iota((rows, rows), 0) < iota((rows, rows), 1)
    place_c = jnp.sum(jnp.where(same & before, 1.0, 0.0), axis=1, keepdims=True)
    place_r = jnp.sum(jnp.where(same & after, 1.0, 0.0), axis=0, keepdims=True)
    target_r = owner_r[0:1] * (2 * CAP) + place_r
    target_c = owner_c * (2 * CAP) + place_c
    row_id = iota((pack_rows, rows), 0).astype(F32)
    low = jnp.where(row_id == target_r, 1.0, 0.0)
    high = jnp.where(row_id == target_r + CAP, 1.0, 0.0)
    both = low + high
    ids_out = jnp.sum(both * local_r[0:1], axis=1, keepdims=True) + adapters * (
        1.0 - jnp.sum(both, axis=1, keepdims=True)
    )

    hid_copy.wait()
    mine = h_all[tp]
    packed = jnp.dot(low.astype(BF16), mine[:, :half], preferred_element_type=F32) + jnp.dot(
        high.astype(BF16), mine[:, half:], preferred_element_type=F32
    )
    packed = packed.reshape(n_ad, 2 * CAP, half).astype(BF16)
    sb[:, :, 0:half] = packed
    sb[:, :, half : half + LANES] = (
        jnp.broadcast_to(ids_out, (pack_rows, LANES)).reshape(n_ad, 2 * CAP, LANES).astype(BF16)
    )

    pl.semaphore_wait(barrier, n_ad - 1 + n_tp - 1)

    row_copies = []
    for i, o in enumerate(ad_peers):
        row_copies.append(
            pltpu.make_async_remote_copy(
                src_ref=sb.at[o], dst_ref=rb.at[ad], send_sem=row_sem.at[0], recv_sem=row_sem.at[1],
                device_id=(o, tp), device_id_type=MESH,
            )
        )
        row_copies[-1].start()
    own_rows = pltpu.make_async_copy(sb.at[ad], rb.at[ad], row_sem.at[1])
    own_rows.start()

    def slab_copy(src, to, n):
        return pltpu.make_async_remote_copy(
            src_ref=h_all.at[src], dst_ref=h_all.at[src], send_sem=slab_sem.at[3], recv_sem=slab_sem.at[n],
            device_id=(ad, to), device_id_type=MESH,
        )

    slab_far = slab_copy(tp, far, 0)
    slab_far.start()
    slab_near = slab_copy(tp, near, 1)
    slab_near.start()

    fill_copy.wait()
    q_copy.wait()
    k_copy.wait()
    v_copy.wait()
    for c in w_copies:
        c.start()

    lane_group = iota((heads, kv * ctx), 1)
    head_row = iota((heads, kv * ctx), 0)
    block_ok = jnp.zeros((heads, kv * ctx), jnp.bool_)
    for g in range(kv):
        block_ok = block_ok | (
            (lane_group >= g * ctx) & (lane_group < (g + 1) * ctx)
            & (head_row >= g * group) & (head_row < (g + 1) * group)
        )
    slot = lane_group
    for g in range(1, kv):
        slot = jnp.where(lane_group >= g * ctx, lane_group - g * ctx, slot)
    slot = jnp.where(block_ok, slot, ctx)

    for b in range(rows):
        p_s[b] = jnp.where(
            slot < fill_ref[b], dot_last(q_s[b], k_s[b].reshape(kv * ctx, head)) * scale, -1e30
        )
    for b in range(rows):
        s = p_s[b]
        m = jnp.max(s, axis=1, keepdims=True)
        p = jnp.exp(s - m)
        p_s[b] = p
        m_s[b] = jnp.broadcast_to(m, (heads, head))
        l_s[b] = jnp.broadcast_to(jnp.sum(p, axis=1, keepdims=True), (heads, head))
    for b in range(rows):
        acc_s[b] = jnp.dot(p_s[b].astype(BF16), v_s[b].reshape(kv * ctx, head), preferred_element_type=F32)

    dn_copy.wait()
    for j in range(slab // LANES):
        dn_t[j * LANES : (j + 1) * LANES] = dn_s[:, j * LANES : (j + 1) * LANES].T

    slab_far.wait_recv()
    slab_on = slab_copy(far, near, 2)
    slab_on.start()

    sub = iota((n_ad, 2 * CAP, LANES), 1).reshape(pack_rows, LANES)
    is_low = sub < CAP
    lane_adapter = jnp.floor(iota((pack_rows, LANES), 1).astype(F32) * (1.0 / rank))
    landed(rb, row_sem.at[1])
    wide = rb[:, :, 0:half].astype(F32).reshape(pack_rows, half)
    ids = rb[:, :, half : half + LANES].astype(F32).reshape(pack_rows, LANES)
    got = wide.astype(BF16)
    squares = jnp.sum(wide * wide, axis=1, keepdims=True)
    latent = jnp.zeros((pack_rows, LANES), F32)
    for t in range(0, groups, 2):
        cols = slice(t * LANES, (t + 2) * LANES)
        first = jnp.dot(got, dn_t[0:half, cols], preferred_element_type=F32)
        second = jnp.dot(got, dn_t[half:slab, cols], preferred_element_type=F32)
        for u in range(2):
            part = slice(u * LANES, (u + 1) * LANES)
            pick = jnp.where(is_low, first[:, part], second[:, part])
            latent = latent + jnp.where(ids == lane_adapter + (t + u) * per, pick, 0.0)
    mine_lane = lane_adapter == ids - per * jnp.floor(ids * (1.0 / per))
    msg = jnp.where(mine_lane, latent, squares).reshape(n_ad, 2 * CAP, LANES)
    pb[tp] = msg[:, 0:CAP] + msg[:, CAP : 2 * CAP]

    lat_copies = []
    for i, t in enumerate(tp_peers):
        lat_copies.append(
            pltpu.make_async_remote_copy(
                src_ref=pb.at[tp], dst_ref=pb.at[tp], send_sem=lat_sem.at[0], recv_sem=lat_sem.at[1],
                device_id=(ad, t), device_id_type=MESH,
            )
        )
        lat_copies[-1].start()

    slab_near.wait_recv()
    slab_on.wait_recv()
    square_sum = jnp.zeros((rows, 1), F32)
    for t in range(n_tp):
        x = h_all[t].astype(F32)
        square_sum = square_sum + jnp.sum(x * x, axis=1, keepdims=True)
    inverse = lax.rsqrt(square_sum / MODEL_WIDTH + epsilon)
    for t in range(n_tp):
        normed = (h_all[t].astype(F32) * inverse).astype(BF16)
        stack = jnp.concatenate([normed[:, j * LANES : (j + 1) * LANES] for j in range(slab // LANES)], axis=0)
        wide_rows = jnp.dot(stack, parity, preferred_element_type=F32).astype(BF16)
        for j in range(slab // LANES):
            at = 2 * (t * slab + j * LANES)
            both = wide_rows[j * rows : (j + 1) * rows]
            lhs_s[0:rows, at : at + 2 * LANES] = both[:, 0 : 2 * LANES]
            lhs_s[rows : 2 * rows, at : at + 2 * LANES] = both[:, 2 * LANES :]
    up_copy.wait()
    up_both = [[], []]
    for t in range(groups):
        flat = columns(up_s[4 * t * LANES : 4 * (t + 1) * LANES])
        for kind in range(2):
            up_both[kind].append(
                lax.dot_general(
                    parity[:, 2 * kind * LANES : 2 * (kind + 1) * LANES], flat, (((1,), (0,)), ((), ())),
                    preferred_element_type=F32,
                ).astype(BF16)
            )
    up_both = [jnp.concatenate(u, axis=0) for u in up_both]

    landed(pb.at[pl.ds(0, n_tp - 1)], lat_sem.at[1])
    total = pb[0]
    for t in range(1, n_tp):
        total = total + pb[t]
    total = jnp.concatenate([total, total], axis=1).reshape(pack_rows, LANES)
    square_sum = jnp.max(jnp.where(mine_lane, 0.0, total), axis=1, keepdims=True)
    latent = total * lax.rsqrt(square_sum / MODEL_WIDTH + epsilon)
    latent = jnp.where(mine_lane, latent, 0.0).astype(BF16)
    spread = jnp.concatenate(
        [jnp.where(ids == lane_adapter + t * per, latent, jnp.zeros_like(latent)) for t in range(groups)], axis=1
    )
    key_delta, value_delta = (jnp.dot(spread, u, preferred_element_type=F32) for u in up_both)
    is_key = iota((n_ad, 2 * CAP, width), 1).reshape(pack_rows, width) < CAP
    delta = adapter_scale * jnp.where(is_key, key_delta, value_delta)
    db[...] = delta.reshape(n_ad, 2 * CAP, width).astype(BF16)

    ret_copies = []
    for i, o in enumerate(ad_peers):
        ret_copies.append(
            pltpu.make_async_remote_copy(
                src_ref=db.at[o], dst_ref=ret.at[ad], send_sem=ret_sem.at[0], recv_sem=ret_sem.at[1],
                device_id=(o, tp), device_id_type=MESH,
            )
        )
        ret_copies[-1].start()
    own_ret = pltpu.make_async_copy(db.at[ad], ret.at[ad], ret_sem.at[1])
    own_ret.start()

    base = jnp.zeros((2 * rows, width), F32)
    piece = slab // 4
    for t in range(n_tp):
        w_copies[t].wait()
        for j in range(4):
            at = t * slab + j * piece
            flat = columns(w_s[4 * at : 4 * (at + piece)])
            base = base + jnp.dot(lhs_s[:, 2 * at : 2 * (at + piece)], flat, preferred_element_type=F32)

    pick_id = iota((rows, pack_rows), 1).astype(F32)
    landed(sb.at[pl.ds(0, n_ad - 1)], row_sem.at[0])
    landed(pb.at[pl.ds(0, n_tp - 1)], lat_sem.at[0])
    landed(h_all.at[pl.ds(0, n_tp - 1)], slab_sem.at[3])
    landed(db.at[pl.ds(0, n_ad - 1)], ret_sem.at[0])
    landed(ret, ret_sem.at[1])
    back = ret[...].astype(F32).reshape(pack_rows, width).astype(BF16)
    pick = jnp.concatenate(
        [jnp.where(pick_id == target_c + kind * CAP, 1.0, 0.0) for kind in range(2)], axis=0
    ).astype(BF16)
    moved = jnp.dot(pick, back, preferred_element_type=F32)
    new = (base + moved).astype(BF16)
    app_ref[0] = new[0:rows]
    app_ref[1] = new[rows : 2 * rows]
    new = new.astype(F32)
    fresh = (new[0:rows], new[rows : 2 * rows])
    for b in range(rows):
        key_rows, value_rows = (
            jnp.concatenate(
                [jnp.broadcast_to(f[b : b + 1, g * head : (g + 1) * head], (group, head)) for g in range(kv)], axis=0
            )
            for f in fresh
        )
        own = jnp.sum(q_s[b].astype(F32) * key_rows, axis=1, keepdims=True) * scale
        m = m_s[b]
        top = jnp.maximum(m, own)
        keep = jnp.exp(m - top)
        own_exp = jnp.exp(own - top)
        ctx_ref[b] = ((acc_s[b] * keep + own_exp * value_rows) / (l_s[b] * keep + own_exp)).astype(BF16)


def by_tile(a):
    tiles = a.shape[-1] // LANES
    return a.reshape(-1, 2, tiles, LANES).transpose(0, 2, 1, 3).reshape(-1, LANES)


def on_device(n_ad, n_tp, hidden, queries, keys, values, fill, choice, weight, down, up):
    rows, slab = hidden.shape
    adapters, rank, _ = down.shape
    width = up.shape[3]
    heads, head = queries.shape[1:]
    kv = keys.shape[1]
    pack_rows = 2 * CAP
    any_spec = pl.BlockSpec(memory_space=pl.ANY)
    vmem = pl.BlockSpec(memory_space=pltpu.VMEM)
    app, ctx = pl.pallas_call(
        functools.partial(kernel, n_ad, n_tp, rank, width),
        out_shape=(
            jax.ShapeDtypeStruct((2, rows, width), BF16),
            jax.ShapeDtypeStruct(queries.shape, BF16),
        ),
        in_specs=[any_spec] * 9,
        out_specs=(vmem, vmem),
        scratch_shapes=[
            pltpu.VMEM((1, rows), jnp.int32),
            pltpu.SMEM((rows,), jnp.int32),
            pltpu.VMEM((n_tp, rows, slab), BF16),
            pltpu.VMEM(queries.shape, BF16),
            pltpu.VMEM(keys.shape, BF16),
            pltpu.VMEM(values.shape, BF16),
            pltpu.VMEM((4 * weight.shape[0], LANES), BF16),
            pltpu.VMEM((adapters * rank, slab), BF16),
            pltpu.VMEM((slab, adapters * rank), BF16),
            pltpu.VMEM((4 * adapters * rank, LANES), BF16),
            pltpu.VMEM((n_ad, pack_rows, slab // 2 + LANES), BF16),
            pltpu.VMEM((n_ad, pack_rows, slab // 2 + LANES), BF16),
            pltpu.VMEM((n_tp, n_ad, CAP, LANES), F32),
            pltpu.VMEM((n_ad, pack_rows, width), BF16),
            pltpu.VMEM((n_ad, pack_rows, width), BF16),
            pltpu.VMEM((2 * rows, 2 * weight.shape[0]), BF16),
            pltpu.VMEM(queries.shape, F32),
            pltpu.VMEM(queries.shape, F32),
            pltpu.VMEM(queries.shape, F32),
            pltpu.VMEM((rows, heads, kv * keys.shape[2]), F32),
            pltpu.SemaphoreType.DMA((8,)),
            pltpu.SemaphoreType.DMA((n_tp,)),
            pltpu.SemaphoreType.DMA((4,)),
            pltpu.SemaphoreType.DMA((2,)),
            pltpu.SemaphoreType.DMA((2,)),
            pltpu.SemaphoreType.DMA((2,)),
        ],
        compiler_params=pltpu.CompilerParams(
            collective_id=0, has_side_effects=True, vmem_limit_bytes=40 * 1024 * 1024
        ),
    )(*[
        pltpu.with_memory_space_constraint(x, pltpu.HBM)
        for x in (
            choice.reshape(1, rows), fill, hidden, queries, keys, values,
            by_tile(weight),
            down.reshape(adapters * rank, slab),
            by_tile(up),
        )
    ])

    def finish(app_ref, ctx_ref, app_out, ctx_out):
        for kind in range(2):
            for g in range(kv):
                app_out[:, kind, g, :] = app_ref[kind, :, g * head : (g + 1) * head]
        ctx_out[...] = ctx_ref[...]

    return pl.pallas_call(
        finish,
        out_shape=(
            jax.ShapeDtypeStruct((rows, 2, kv, head), BF16),
            jax.ShapeDtypeStruct(queries.shape, BF16),
        ),
        in_specs=[vmem] * 2,
        out_specs=(vmem, vmem),
        compiler_params=pltpu.CompilerParams(vmem_limit_bytes=4 * 1024 * 1024),
    )(app, ctx)


def solution(mesh):
    placed = (
        P("ad", "tp"),
        P("ad", "tp", None),
        P("ad", "tp", None, None),
        P("ad", "tp", None, None),
        P("ad"),
        P("ad"),
        P(None, None, "tp"),
        P("ad", None, "tp"),
        P("ad", None, None, "tp"),
    )
    return jax.shard_map(
        functools.partial(on_device, mesh.shape["ad"], mesh.shape["tp"]),
        mesh=mesh,
        in_specs=placed,
        out_specs=(P("ad", None, "tp", None), P("ad", "tp", None)),
        check_vma=False,
    )
```
